256 devices in a mesh: elem: 16 (over z, core), front: 16 (over y, x).
Axes of the slice: x: 4, y: 4, z: 8, core: 2. Of those that a mesh axis runs over, the one named last changes fastest.
Arguments:
- elem_mat: bfloat16 [24, 24, 32768], P(None, None, ('elem', 'front')), may hold values from -1.25 to 1.25
- elem_deriv: bfloat16 [24, 24, 32768], P(None, None, ('elem', 'front')), may hold values from -1.1953125 to 1.1953125
- elem_disp: bfloat16 [24, 32768], P(None, ('elem', 'front')), may hold values from -6 to 6
- elem_sens: bfloat16 [32768, 24, 512], P(('elem', 'front')), may hold values from -3 to 3
- design_var: int32 [32768], P(('elem', 'front')), may hold values from 0 to 511
- dof_rows: int32 [24, 32768], P(None, ('elem', 'front')), may hold values from 0 to 3584, as said below
- inverse_factor: bfloat16 [57344, 8192], P('front', 'elem'), may hold values from -2 to 2
- coupling: bfloat16 [8192, 49152], P('elem', 'front'), may hold values from -0.0625 to 0.0625
- front_sizes: int32 [7], replicated, may hold values from 4096 to 8192
Outputs:
- sens: float32 [57344, 512], P('front', 'elem')
The draws below stay inside these ranges and needn't reach their ends.
Inputs may be any that keep to these rules, and one draw needn't show every extreme that they name: `dof_rows`: the used rows of one element lie in one aligned block of 128 rows; the value 3584 marks a degree of freedom that no front holds.
All inputs are finite; a program needn't handle non-finite values.
Results may differ from the reference program's by a relative error of at most 0.014.
Values may be sent and summed in bfloat16 or wider, within the bound.
No kernel may reach another device: no remote copies, remote signals or barrier semaphores. Data moves between devices by JAX's collectives and lax.ppermute only.
A program may use at most 128 MiB of HBM per device.

```python
import jax
import jax.numpy as jnp
from jax import lax

DOF = 24
NRHS = 512
FS = 8192
LEVELS = 3
BLK = 128
E_DEV = 128
ELEMS = 32768
LR = 3584
CR = 3072
FRONTS = 7
N_FRONT = 16


def draw_dof_rows(key, part):
    key_block = jax.random.fold_in(key, 11)
    key_offset = jax.random.fold_in(key, 12)
    key_unused = jax.random.fold_in(key, 13)
    block_index = jax.random.randint(key_block, (1, ELEMS), 0, LR // BLK)
    offsets = jax.random.randint(key_offset, (DOF, ELEMS), 0, BLK)
    unused = jax.random.randint(key_unused, (DOF, ELEMS), 0, 8)
    places = block_index * BLK + offsets
    return jnp.where(unused == 0, LR, places).astype(jnp.int32)


def draw_inverse_factor(key, part):
    total_rows = N_FRONT * LR
    row_at = jnp.arange(total_rows, dtype=jnp.int32)
    device_at = row_at // LR
    spot_at = row_at % LR
    global_row = jnp.zeros_like(row_at)
    start_spot = 0
    for level_at in range(LEVELS):
        share_count = N_FRONT >> LEVELS - 1 - level_at
        block_rows = FS // share_count
        inside = (spot_at >= start_spot) & (spot_at < start_spot + block_rows)
        global_row = jnp.where(inside, device_at % share_count * block_rows + spot_at - start_spot, global_row)
        start_spot = start_spot + block_rows
    key_off = jax.random.fold_in(key, 21)
    key_diag = jax.random.fold_in(key, 22)
    spread_part = jax.random.normal(key_off, (total_rows, FS), jnp.float32) * (0.5 / FS ** 0.5)
    diag_part = jax.random.uniform(key_diag, (total_rows,), jnp.float32, 0.6, 1.2)
    spread_part = jnp.clip(spread_part, -1.0, 1.0)
    columns_at = jnp.arange(FS, dtype=jnp.int32)
    on_diag = (columns_at[None, :] == global_row[:, None]).astype(jnp.float32)
    return (spread_part * (1.0 - on_diag) + on_diag * diag_part[:, None]).astype(jnp.bfloat16)


def place_ends(result, key, least, largest):
    spot = [jax.random.randint(jax.random.fold_in(key, axis), (), 0, length) for axis, length in enumerate(result.shape)]
    widest = result.shape.index(max(result.shape))
    next_to = spot[:widest] + [(spot[widest] + 1) % result.shape[widest]] + spot[widest + 1:]
    return result.at[tuple(spot)].set(least).at[tuple(next_to)].set(largest)


def block_scale(stream_key, dims, cuts, least, high):
    factor_of, own = 1.0, jax.random.fold_in(stream_key, 6)
    for position, blocks in cuts:
        draws = jnp.exp(jax.random.uniform(jax.random.fold_in(own, position), (blocks,), jnp.float32, least / len(cuts), high / len(cuts)))
        factor_of = factor_of * jnp.repeat(draws, dims[position] // blocks).reshape([-1 if axis == position else 1 for axis in range(len(dims))])
    return factor_of


def gaussian(rng, extent, scale, reach, shards=(), kind=jnp.bfloat16):
    entries = jax.random.normal(rng, extent, jnp.float32) * scale
    if len(shards) > 0:
        entries = block_scale(rng, extent, shards, -0.22, 0.18) * entries
    return jnp.clip(entries, min=-reach, max=reach).astype(kind)


def setup_inputs(seed: int = 0) -> dict:
    key_of = jax.random.split(jax.random.key(seed), 10)
    return {
        "elem_mat": gaussian(key_of[0], (DOF, DOF, ELEMS), DOF ** -0.5, 1.25, ((2, 256),)),
        "elem_deriv": gaussian(key_of[1], (DOF, DOF, ELEMS), 0.2, 1.1953125, ((2, 256),)),
        "elem_disp": gaussian(key_of[2], (DOF, ELEMS), 1.0, 6.0, ((1, 256),)),
        "elem_sens": gaussian(key_of[3], (ELEMS, DOF, NRHS), 0.5, 3.0, ((0, 256),)),
        "design_var": place_ends(jax.random.randint(key_of[4], (ELEMS,), 0, NRHS), jax.random.fold_in(key_of[4], 1), 0, NRHS - 1).astype(jnp.int32),
        "dof_rows": draw_dof_rows(jax.random.fold_in(key_of[9], 71), 0),
        "inverse_factor": draw_inverse_factor(jax.random.fold_in(key_of[9], 71), 0),
        "coupling": gaussian(key_of[7], (FS, N_FRONT * CR), FS ** -0.5, 0.0625, ((0, 16), (1, 16))),
        "front_sizes": place_ends(jax.random.randint(key_of[8], (FRONTS,), FS // 2, FS + 1), jax.random.fold_in(key_of[8], 1), FS // 2, FS).astype(jnp.int32),
    }


def level_shape(level_at):
    share_count = N_FRONT >> (LEVELS - 1 - level_at)
    return share_count, FS // share_count


def level_offset(level_at):
    return sum(level_shape(other)[1] for other in range(level_at))


def take_level(matrix, level_at):
    share_count, block_rows = level_shape(level_at)
    offset = level_offset(level_at)
    sliced = matrix.reshape(N_FRONT, LR, matrix.shape[-1])[:, offset:offset + block_rows]
    return sliced.reshape(N_FRONT // share_count, FS, matrix.shape[-1])


def couple_level(coupling, level_at):
    share_count, block_rows = level_shape(level_at)
    offset = level_offset(level_at)
    sliced = coupling.reshape(FS, N_FRONT, CR)[:, :, offset:offset + block_rows]
    return sliced.reshape(FS, N_FRONT // share_count, FS).transpose(1, 0, 2)


def level_mask(front_sizes, level_at):
    front_count = 2 ** (LEVELS - 1 - level_at)
    first_front = sum(2 ** (LEVELS - 1 - other) for other in range(level_at))
    live_sizes = front_sizes[first_front:first_front + front_count]
    rows_at = jnp.arange(FS, dtype=jnp.int32)
    return (rows_at[None, :, None] < live_sizes[:, None, None]).astype(jnp.float32)


def reference(elem_mat, elem_deriv, elem_disp, elem_sens, design_var, dof_rows, inverse_factor, coupling, front_sizes):
    def add_block(totals, block_index):
        start_row = block_index * E_DEV
        tables = lax.dynamic_slice_in_dim(elem_mat, start_row, E_DEV, 2).astype(jnp.float32)
        derivs = lax.dynamic_slice_in_dim(elem_deriv, start_row, E_DEV, 2).astype(jnp.float32)
        disps = lax.dynamic_slice_in_dim(elem_disp, start_row, E_DEV, 1).astype(jnp.float32)
        sens_block = lax.dynamic_slice_in_dim(elem_sens, start_row, E_DEV, 0).astype(jnp.float32)
        variables = lax.dynamic_slice_in_dim(design_var, start_row, E_DEV, 0)
        places = lax.dynamic_slice_in_dim(dof_rows, start_row, E_DEV, 1).T
        pseudo = -jnp.einsum("ije,ejc->eic", tables, sens_block)
        drive_term = -jnp.einsum("ije,je->ei", derivs, disps)
        hit_column = (jnp.arange(NRHS, dtype=jnp.int32)[None, :] == variables[:, None]).astype(jnp.float32)
        pseudo = pseudo + drive_term[:, :, None] * hit_column[:, None, :]
        front_index = block_index % N_FRONT
        places = jnp.where(places < LR, places + front_index * LR, N_FRONT * LR).astype(jnp.int32)
        totals = totals.at[places.reshape(-1)].add(pseudo.reshape(-1, NRHS), mode="drop")
        return totals, None

    start_loads = jnp.zeros((N_FRONT * LR, NRHS), jnp.float32)
    loads, _ = lax.scan(add_block, start_loads, jnp.arange(ELEMS // E_DEV, dtype=jnp.int32))

    forward_out = []
    acc_rows = None
    for level_at in range(LEVELS):
        live_rows = level_mask(front_sizes, level_at)
        factor_rows = take_level(inverse_factor, level_at).astype(jnp.float32)
        given = take_level(loads, level_at)
        if acc_rows is not None:
            given = given - acc_rows
        rhs_in = (live_rows * given).astype(jnp.bfloat16)
        solved = live_rows * jnp.einsum("nij,njc->nic", factor_rows, rhs_in.astype(jnp.float32))
        forward_out.append(solved)
        if level_at < LEVELS - 1:
            links = couple_level(coupling, level_at).astype(jnp.float32)
            rounded = solved.astype(jnp.bfloat16).astype(jnp.float32)
            partial_value = jnp.einsum("nij,njc->nic", links, rounded)
            acc_rows = partial_value.reshape(partial_value.shape[0] // 2, 2, FS, NRHS).sum(axis=1)

    pieces_out = [None] * LEVELS
    parent_rows = None
    for level_at in reversed(range(LEVELS)):
        live_rows = level_mask(front_sizes, level_at)
        factor_rows = take_level(inverse_factor, level_at).astype(jnp.float32)
        residual = forward_out[level_at]
        if parent_rows is not None:
            links = couple_level(coupling, level_at).astype(jnp.float32)
            spread_parent = jnp.repeat(parent_rows.astype(jnp.float32), 2, axis=0)
            residual = residual - jnp.einsum("nji,njc->nic", links, spread_parent)
        back_in = (live_rows * residual).astype(jnp.bfloat16)
        answer = live_rows * jnp.einsum("nji,njc->nic", factor_rows, back_in.astype(jnp.float32))
        pieces_out[level_at] = answer
        parent_rows = answer.astype(jnp.bfloat16)

    laid_out = [pieces_out[level_at].reshape(N_FRONT, level_shape(level_at)[1], NRHS) for level_at in range(LEVELS)]
    return jnp.concatenate(laid_out, axis=1).reshape(N_FRONT * LR, NRHS)
```

```python
import jax
import jax.numpy as jnp
from jax import lax
from jax.sharding import Mesh
from jax.sharding import PartitionSpec as P

FS = 8192
LR = 3584
NRHS = 512
BF = jnp.bfloat16
F32 = jnp.float32

Z, C, H, L, X = "z", "c", "h", "l", "x"
FRONT = (H, L, X)
PAIR = (L, X)


def dot_t(a, b):
    return lax.dot_general(a, b, (((1,), (1,)), ((), ())), preferred_element_type=F32)


def dot(a, b):
    return lax.dot_general(a, b, (((1,), (0,)), ((), ())), preferred_element_type=F32)


def exchange(chunks, axes):
    return lax.all_to_all(chunks, axes, split_axis=0, concat_axis=0, tiled=True)


def reduce_chunks(chunks, axes):
    return jnp.sum(exchange(chunks.astype(BF), axes).astype(F32), axis=0)


def gather_chunks(chunk, axes, count):
    return exchange(jnp.broadcast_to(chunk[None], (count,) + chunk.shape), axes)


def form_loads(tables, derivs, disps, sens_block, variables, places):
    pseudo = -jnp.einsum("ije,ejc->eic", tables, sens_block, preferred_element_type=F32)
    drive_term = -jnp.einsum("ije,je->ei", derivs, disps, preferred_element_type=F32)
    column_ids = lax.iota(jnp.int32, NRHS)
    hit_column = (column_ids[None, :] == variables[:, None]).astype(F32)
    pseudo = pseudo + drive_term[:, :, None] * hit_column[:, None, :]
    term_rows = jnp.zeros((LR, NRHS), F32)
    return term_rows.at[places.T.reshape(-1)].add(pseudo.reshape(-1, NRHS), mode="drop")


def pair_up(is_first, own, other, axis):
    first = jnp.where(is_first, own, other)
    second = jnp.where(is_first, other, own)
    return jnp.concatenate([first, second], axis)


def body(
    elem_mat,
    elem_deriv,
    elem_disp,
    elem_sens,
    design_var,
    dof_rows,
    inverse_factor,
    coupling,
    front_sizes,
):
    z = lax.axis_index(Z)
    c = lax.axis_index(C)
    h = lax.axis_index(H)
    l = lax.axis_index(L)
    x = lax.axis_index(X)
    core_swap = [(0, 1), (1, 0)]
    is_c0 = c == 0

    w0 = lax.all_gather(inverse_factor[0:2048], (C, X), axis=0, tiled=False).reshape(2, FS, 512)
    g0 = lax.all_gather(coupling[:, 0:2048], (C, X), axis=0, tiled=False).reshape(2, 4, 512, 2048)
    w2 = lax.all_gather(inverse_factor[3072:3584], (C, H, L, X), axis=0, tiled=False).reshape(2, FS, 512)
    w1_own = inverse_factor[2048:3072]
    g1_own = coupling[:, 2048:3072]
    w1_other = lax.ppermute(w1_own, C, core_swap)
    g1_other = lax.ppermute(g1_own, C, core_swap)

    block_rows = z * 1024 + lax.iota(jnp.int32, 1024)

    def mask_of(front, rows):
        size = lax.dynamic_index_in_dim(front_sizes, front, 0, keepdims=False)
        return (rows < size).astype(F32)[None, :]

    mask0 = mask_of(h * 2 + l, block_rows)
    mask1 = mask_of(4 + h, block_rows)
    mask1f = mask_of(4 + h, (l * 4 + x) * 1024 + lax.iota(jnp.int32, 1024))
    mask2 = mask_of(6, block_rows)

    term_rows = form_loads(elem_mat, elem_deriv, elem_disp, elem_sens, design_var, dof_rows)
    term_cols = term_rows.astype(BF).T.reshape(8, 2, 32, LR)
    halves = exchange(term_cols.transpose(1, 0, 2, 3), C).astype(F32)
    half = halves[0] + halves[1]
    top = half[:, :, :2048].astype(BF).reshape(2, 4, 32, 2048).transpose(1, 0, 2, 3)
    top = exchange(top, X)
    top = top.reshape(4, 2, 32, 2, 1024).transpose(0, 3, 1, 2, 4).reshape(8, 64, 1024)
    load0 = reduce_chunks(top, Z)

    rest = lax.psum_scatter(half[:, :, 2048:], Z, scatter_dimension=0, tiled=True)[0]
    turn = [(zz * 8 + ss, ss * 8 + zz) for zz in range(8) for ss in range(8)]
    load1 = lax.ppermute(rest[:, :1024], (Z, L, X), turn)
    rest2 = rest[:, 1024:].reshape(2, 16, 512)
    is_even = (x & 1) == 0
    got = []
    for k in range(2):
        sent = jnp.where(is_even, rest2[k], rest2[1 - k])
        perm = [
            (zz * 16 + ff, (ff >> 1) * 16 + ((ff & 1) ^ k) * 8 + zz)
            for zz in range(8)
            for ff in range(16)
        ]
        got.append(lax.ppermute(sent, (Z, H, L, X), perm))
    load2 = pair_up(h == 0, got[0], got[1], 1)

    rhs0 = (mask0 * load0).astype(BF)
    y0_part = dot_t(rhs0[:, :512], w0[0]) + dot_t(rhs0[:, 512:], w0[1])
    y0 = mask0 * reduce_chunks(y0_part.reshape(64, 8, 1024).transpose(1, 0, 2), Z)
    y0_all = gather_chunks(y0.astype(BF), Z, 8).transpose(1, 0, 2).reshape(64, FS)
    acc0 = []
    for at in range(2):
        acc0.append(
            sum(dot_t(y0_all[:, s * 2048 : s * 2048 + 2048], g0[at, s]) for s in range(4))
        )
    acc0 = jnp.concatenate(acc0, 1).reshape(2, 32, 1024)
    is_l0 = l == 0
    acc0_kept = jnp.where(is_l0, acc0[0], acc0[1])
    acc0_sent = jnp.where(is_l0, acc0[1], acc0[0])
    acc0_sum = acc0_kept + lax.ppermute(acc0_sent, L, core_swap)

    rhs1 = (mask1 * (load1 - acc0_sum)).astype(BF)
    rhs1 = gather_chunks(rhs1, PAIR, 8).reshape(256, 1024)

    def by_core(value):
        return (
            jnp.where(is_c0, value[:, :512], value[:, 512:]),
            jnp.where(is_c0, value[:, 512:], value[:, :512]),
        )

    rhs1_own, rhs1_other = by_core(rhs1)
    y1_part = dot_t(rhs1_own, w1_own) + dot_t(rhs1_other, w1_other)
    y1 = mask1f * reduce_chunks(y1_part.reshape(8, 32, 1024), Z)
    y1_all = gather_chunks(y1.astype(BF), Z, 8).reshape(256, 1024)
    acc1 = pair_up(is_c0, dot_t(y1_all, g1_own).astype(BF), dot_t(y1_all, g1_other).astype(BF), 1)
    acc1 = acc1.reshape(8, 2, 16, 1024).transpose(1, 0, 2, 3).reshape(16, 16, 1024)
    acc1_sum = reduce_chunks(acc1, FRONT)

    rhs2 = (mask2 * (load2 - acc1_sum)).astype(BF)
    y2_part = dot_t(rhs2[:, :512], w2[0]) + dot_t(rhs2[:, 512:], w2[1])
    y2 = mask2 * reduce_chunks(y2_part.reshape(16, 8, 1024).transpose(1, 0, 2), Z)
    back2 = gather_chunks(y2.astype(BF), Z, 8).transpose(1, 0, 2).reshape(16, FS)
    x2 = mask2 * jnp.concatenate([dot(back2, w2[0]), dot(back2, w2[1])], 1)
    got = []
    for k in range(2):
        sent = jnp.where((h ^ k) == 0, x2[:, :512], x2[:, 512:])
        perm = [
            (zz * 16 + ff, (ff & 7) * 16 + 2 * zz + ((ff >> 3) ^ k))
            for zz in range(8)
            for ff in range(16)
        ]
        got.append(lax.ppermute(sent, (Z, H, L, X), perm))
    out2 = pair_up(is_even, got[0], got[1], 0)
    x2_all = gather_chunks(x2.astype(BF), FRONT, 16)
    x2_all = x2_all.reshape(2, 8, 16, 1024).transpose(1, 0, 2, 3).reshape(256, 1024)

    x2_own, x2_other = by_core(x2_all)
    corr1 = dot(x2_own, g1_own) + dot(x2_other, g1_other)
    z1 = y1 - reduce_chunks(corr1.reshape(8, 32, 1024), Z)
    back1 = gather_chunks((mask1f * z1).astype(BF), Z, 8).reshape(256, 1024)
    x1_part = pair_up(is_c0, dot(back1, w1_own).astype(BF), dot(back1, w1_other).astype(BF), 1)
    x1 = mask1 * reduce_chunks(x1_part.reshape(8, 32, 1024), PAIR)
    out1 = lax.ppermute(x1, (Z, L, X), turn)
    x1_round = x1.astype(BF)
    x1_pair = pair_up(is_l0, x1_round, lax.ppermute(x1_round, L, core_swap), 0)

    corr0 = []
    for s in range(4):
        corr0.append(dot(x1_pair[:, :512], g0[0, s]) + dot(x1_pair[:, 512:], g0[1, s]))
    corr0 = jnp.stack(corr0, 0).reshape(4, 64, 2, 1024).transpose(0, 2, 1, 3).reshape(8, 64, 1024)
    z0 = y0 - reduce_chunks(corr0, Z)
    back0 = gather_chunks((mask0 * z0).astype(BF), Z, 8).transpose(1, 0, 2).reshape(64, FS)
    x0 = mask0 * jnp.concatenate([dot(back0, w0[0]), dot(back0, w0[1])], 1)
    x0 = x0.reshape(2, 32, 1024)
    got = []
    for k in range(2):
        sent = jnp.where(((z & 1) ^ k) == 0, x0[0], x0[1])
        perm = [
            (zz * 4 + xx, (xx + 4 * ((zz & 1) ^ k)) * 4 + (zz >> 1))
            for zz in range(8)
            for xx in range(4)
        ]
        got.append(lax.ppermute(sent, (Z, X), perm))
    out0 = pair_up(z < 4, got[0], got[1], 1)
    return jnp.concatenate([out0, out1, out2], 1).T


def solution(mesh):
    fine = Mesh(mesh.devices.reshape(8, 2, 2, 2, 4), (Z, C, H, L, X))
    elem, front = (Z, C), (H, L, X)
    both = elem + front
    return jax.shard_map(
        body,
        mesh=fine,
        in_specs=(
            P(None, None, both),
            P(None, None, both),
            P(None, both),
            P(both, None, None),
            P(both),
            P(None, both),
            P(front, elem),
            P(elem, front),
            P(),
        ),
        out_specs=P(front, elem),
        check_vma=False,
    )
```

```python
import jax
import jax.numpy as jnp
from jax import lax
from jax.experimental import pallas as pl
from jax.experimental.pallas import tpu as pltpu
from jax.sharding import Mesh
from jax.sharding import PartitionSpec as P

LR = 3584
NRHS = 512
BF = jnp.bfloat16
F32 = jnp.float32
E_STEP = 16
UNROLL = 8

Z, C, H, L, X = "z", "c", "h", "l", "x"
FRONT = (H, L, X)
PAIR = (L, X)


def dot_t(a, b):
    return lax.dot_general(a, b, (((1,), (1,)), ((), ())), preferred_element_type=F32)


def dot(a, b):
    return lax.dot_general(a, b, (((1,), (0,)), ((), ())), preferred_element_type=F32)


def exchange(chunks, axes):
    return lax.all_to_all(chunks, axes, split_axis=0, concat_axis=0, tiled=True)


def reduce_chunks(chunks, axes):
    return jnp.sum(exchange(chunks.astype(BF), axes).astype(F32), axis=0)


def gather_chunks(chunk, axes, count):
    return exchange(jnp.broadcast_to(chunk[None], (count,) + chunk.shape), axes)


def pair_up(is_first, own, other, axis):
    first = jnp.where(is_first, own, other)
    second = jnp.where(is_first, other, own)
    return jnp.concatenate([first, second], axis)


def loads_kernel(block_ref, var_ref, dofs_ref, table_ref, sens_ref, out_ref, total):
    step = pl.program_id(0)

    @pl.when(step == 0)
    def _():
        total[...] = jnp.zeros_like(total)

    row_at = lax.broadcasted_iota(jnp.int32, (128, 24), 0)
    lane_at = lax.broadcasted_iota(jnp.int32, (128, 128), 1)

    def group(index, carry):
        first = index * UNROLL
        spread = []
        for k in range(UNROLL):
            at = first + k
            start = block_ref[step * E_STEP + at] * 128
            hits = (dofs_ref[at] == row_at + start).astype(F32).astype(BF)
            spread.append(jnp.dot(hits, table_ref[at], preferred_element_type=F32))
        for k in range(UNROLL):
            at = first + k
            start = pl.multiple_of(block_ref[step * E_STEP + at] * 128, 128)
            rows = pl.ds(start, 128)
            part = jnp.dot(spread[k][:, :24].astype(BF), sens_ref[at], preferred_element_type=F32)
            total[rows, :] += part
            var = var_ref[step * E_STEP + at]
            tile = pl.ds(pl.multiple_of((var // 128) * 128, 128), 128)
            drive = spread[k][:, 24:25] + spread[k][:, 25:26] + spread[k][:, 26:27]
            total[rows, tile] += jnp.where(lane_at == var % 128, drive, 0.0)
        return carry

    lax.fori_loop(0, E_STEP // UNROLL, group, 0)

    @pl.when(step == pl.num_programs(0) - 1)
    def _():
        def turn(block, carry):
            rows = pl.ds(pl.multiple_of(block * 128, 128), 128)
            for q in range(4):
                tile = total[rows, q * 128 : q * 128 + 128].T.astype(BF)
                for k in range(4):
                    out_ref[k % 2, 2 * q + k // 2, :, rows] = tile[k * 32 : k * 32 + 32]
            return carry

        lax.fori_loop(0, LR // 128, turn, 0)


def form_loads(tables, derivs, disps, sens_block, variables, places):
    drive = jnp.sum(derivs.astype(F32) * disps.astype(F32)[None], axis=1)
    high = lax.reduce_precision(drive, 8, 7)
    middle = lax.reduce_precision(drive - high, 8, 7)
    low = drive - high - middle
    extra = -jnp.stack([high, middle, low], 1).astype(BF)
    fill = jnp.zeros((24, 5, 128), BF)
    table = jnp.concatenate([-tables, extra, fill], 1).transpose(2, 0, 1)
    blocks = jnp.minimum(jnp.min(places, axis=0) // 128, LR // 128 - 1)
    dofs = places.T[:, None, :]
    smem = pl.BlockSpec(memory_space=pltpu.SMEM)
    return pl.pallas_call(
        loads_kernel,
        grid=(128 // E_STEP,),
        in_specs=[
            smem,
            smem,
            pl.BlockSpec((E_STEP, 1, 24), lambda i: (i, 0, 0)),
            pl.BlockSpec((E_STEP, 24, 32), lambda i: (i, 0, 0)),
            pl.BlockSpec((E_STEP, 24, NRHS), lambda i: (i, 0, 0)),
        ],
        out_specs=pl.BlockSpec((2, 8, 32, LR), lambda i: (0, 0, 0, 0)),
        out_shape=jax.ShapeDtypeStruct((2, 8, 32, LR), BF),
        scratch_shapes=[pltpu.VMEM((LR, NRHS), F32)],
        cost_estimate=pl.CostEstimate(flops=800_000_000, bytes_accessed=8_000_000, transcendentals=0),
        name="loads",
    )(blocks, variables, dofs, table, sens_block)


def body(
    elem_mat,
    elem_deriv,
    elem_disp,
    elem_sens,
    design_var,
    dof_rows,
    inverse_factor,
    coupling,
    front_sizes,
):
    z = lax.axis_index(Z)
    c = lax.axis_index(C)
    h = lax.axis_index(H)
    l = lax.axis_index(L)
    x = lax.axis_index(X)
    core_swap = [(0, 1), (1, 0)]

    w_own, g_own = inverse_factor, coupling
    w_other = lax.ppermute(w_own, C, core_swap)
    g_other = lax.ppermute(g_own, C, core_swap)

    def turned(value):
        return jnp.where(c == 0, value, jnp.concatenate([value[:, 512:], value[:, :512]], 1))

    count = lax.iota(jnp.int32, 1024)
    block_rows = z * 1024 + jnp.where(c == 0, count, count ^ 512)

    def mask_of(front, rows):
        size = lax.dynamic_index_in_dim(front_sizes, front, 0, keepdims=False)
        return (rows < size).astype(F32)[None, :]

    place = l * 4 + x
    mask0 = mask_of(h * 2 + l, block_rows)
    mask0f = mask_of(h * 2 + l, x * 2048 + lax.iota(jnp.int32, 2048))
    mask1 = mask_of(4 + h, block_rows)
    mask1f = mask_of(4 + h, place * 1024 + count)
    mask2 = mask_of(6, block_rows)
    mask2f = mask_of(6, h * 4096 + place * 512 + lax.iota(jnp.int32, 512))

    def times_w(rhs, first, last):
        return dot_t(rhs[:, :512], w_own[first:last]) + dot_t(rhs[:, 512:], w_other[first:last])

    def times_wt(back, first, last):
        parts = [dot(back, w[first:last]).astype(BF) for w in (w_own, w_other)]
        return jnp.concatenate(parts, 1)

    def times_g(y, first, last):
        parts = [dot_t(y, g[:, first:last]).astype(BF) for g in (g_own, g_other)]
        return jnp.concatenate(parts, 1)

    def times_gt(parent, first, last):
        return dot(parent[:, :512], g_own[:, first:last]) + dot(parent[:, 512:], g_other[:, first:last])

    def by_front(value):
        return value.reshape(8, 2, 16, 1024).transpose(1, 0, 2, 3).reshape(16, 16, 1024)

    def from_front(value):
        return value.reshape(2, 8, 16, 1024).transpose(1, 0, 2, 3).reshape(256, 1024)

    halves = form_loads(elem_mat, elem_deriv, elem_disp, elem_sens, design_var, dof_rows)
    halves = exchange(halves, C).astype(F32)
    half = halves[0] + halves[1]
    top = exchange(half[:, :, :2048].astype(BF).reshape(4, 64, 2048), X)
    top = top.reshape(4, 64, 2, 1024).transpose(0, 2, 1, 3).reshape(8, 64, 1024)
    load0 = turned(reduce_chunks(top, Z))

    rest = lax.psum_scatter(half[:, :, 2048:], Z, scatter_dimension=0, tiled=True)[0]
    turn = [(zz * 8 + ss, ss * 8 + zz) for zz in range(8) for ss in range(8)]
    load1 = turned(lax.ppermute(rest[:, :1024], (Z, L, X), turn))
    rest2 = rest[:, 1024:].reshape(2, 16, 512)
    is_even = (x & 1) == 0
    got = []
    for k in range(2):
        sent = jnp.where(is_even, rest2[k], rest2[1 - k])
        perm = [
            (zz * 16 + ff, (ff >> 1) * 16 + ((ff & 1) ^ k) * 8 + zz)
            for zz in range(8)
            for ff in range(16)
        ]
        got.append(lax.ppermute(sent, (Z, H, L, X), perm))
    load2 = pair_up((h ^ c) == 0, got[0], got[1], 1)

    rhs0 = gather_chunks((mask0 * load0).astype(BF), X, 4).reshape(256, 1024)
    y0 = mask0f * reduce_chunks(times_w(rhs0, 0, 2048).reshape(8, 32, 2048), Z)
    y0_all = gather_chunks(y0.astype(BF), Z, 8).reshape(256, 2048)
    acc0 = reduce_chunks(times_g(y0_all, 0, 2048).reshape(8, 32, 1024), PAIR)

    rhs1 = gather_chunks((mask1 * (load1 - acc0)).astype(BF), PAIR, 8).reshape(256, 1024)
    y1 = mask1f * reduce_chunks(times_w(rhs1, 2048, 3072).reshape(8, 32, 1024), Z)
    y1_all = gather_chunks(y1.astype(BF), Z, 8).reshape(256, 1024)
    acc1 = reduce_chunks(by_front(times_g(y1_all, 2048, 3072)), FRONT)

    rhs2 = from_front(gather_chunks((mask2 * (load2 - acc1)).astype(BF), FRONT, 16))
    y2 = mask2f * reduce_chunks(times_w(rhs2, 3072, 3584).reshape(8, 32, 512), Z)
    back2 = gather_chunks(y2.astype(BF), Z, 8).reshape(256, 512)
    x2 = mask2 * reduce_chunks(by_front(times_wt(back2, 3072, 3584)), FRONT)
    got = []
    for k in range(2):
        sent = jnp.where((h ^ k ^ c) == 0, x2[:, :512], x2[:, 512:])
        perm = [
            (zz * 16 + ff, (ff & 7) * 16 + 2 * zz + ((ff >> 3) ^ k))
            for zz in range(8)
            for ff in range(16)
        ]
        got.append(lax.ppermute(sent, (Z, H, L, X), perm))
    out2 = pair_up(is_even, got[0], got[1], 0)
    x2_all = from_front(gather_chunks(x2.astype(BF), FRONT, 16))

    z1 = y1 - reduce_chunks(times_gt(x2_all, 2048, 3072).reshape(8, 32, 1024), Z)
    back1 = gather_chunks((mask1f * z1).astype(BF), Z, 8).reshape(256, 1024)
    x1 = mask1 * reduce_chunks(times_wt(back1, 2048, 3072).reshape(8, 32, 1024), PAIR)
    out1 = lax.ppermute(turned(x1), (Z, L, X), turn)
    x1_all = gather_chunks(x1.astype(BF), PAIR, 8).reshape(256, 1024)

    z0 = y0 - reduce_chunks(times_gt(x1_all, 0, 2048).reshape(8, 32, 2048), Z)
    back0 = gather_chunks((mask0f * z0).astype(BF), Z, 8).reshape(256, 2048)
    x0 = mask0 * reduce_chunks(times_wt(back0, 0, 2048).reshape(4, 64, 1024), X)
    x0 = turned(x0).reshape(2, 32, 1024)
    got = []
    for k in range(2):
        sent = jnp.where(((z & 1) ^ k) == 0, x0[0], x0[1])
        perm = [
            (zz * 4 + xx, (2 * xx + ((zz & 1) ^ k)) * 4 + (zz >> 1))
            for zz in range(8)
            for xx in range(4)
        ]
        got.append(lax.ppermute(sent, (Z, X), perm))
    out0 = pair_up((z & 1) == 0, got[0], got[1], 1)
    return jnp.concatenate([out0, out1, out2], 1).T


def solution(mesh):
    fine = Mesh(mesh.devices.reshape(8, 2, 2, 2, 4), (Z, C, H, L, X))
    elem, front = (Z, C), (H, L, X)
    both = elem + front
    return jax.shard_map(
        body,
        mesh=fine,
        in_specs=(
            P(None, None, both),
            P(None, None, both),
            P(None, both),
            P(both, None, None),
            P(both),
            P(None, both),
            P(front, elem),
            P(elem, front),
            P(),
        ),
        out_specs=P(front, elem),
        check_vma=False,
    )
```

```python
import jax
import jax.numpy as jnp
from jax import lax
from jax.experimental import pallas as pl
from jax.experimental.pallas import tpu as pltpu
from jax.sharding import Mesh
from jax.sharding import PartitionSpec as P

LR = 3584
NRHS = 512
BF = jnp.bfloat16
F32 = jnp.float32
E_STEP = 16
UNROLL = 8

Z, C, H, L, X = "z", "c", "h", "l", "x"
FRONT = (H, L, X)
PAIR = (L, X)


def dot_t(a, b):
    return lax.dot_general(a, b, (((1,), (1,)), ((), ())), preferred_element_type=F32)


def dot(a, b):
    return lax.dot_general(a, b, (((1,), (0,)), ((), ())), preferred_element_type=F32)


def exchange(chunks, axes):
    return lax.all_to_all(chunks, axes, split_axis=0, concat_axis=0, tiled=True)


def reduce_chunks(chunks, axes):
    return jnp.sum(exchange(chunks.astype(BF), axes).astype(F32), axis=0)


def gather_chunks(chunk, axes, count):
    return exchange(jnp.broadcast_to(chunk[None], (count,) + chunk.shape), axes)


def pair_up(is_first, own, other, axis):
    first = jnp.where(is_first, own, other)
    second = jnp.where(is_first, other, own)
    return jnp.concatenate([first, second], axis)


def loads_kernel(block_ref, var_ref, dofs_ref, table_ref, sens_ref, out_ref, total):
    step = pl.program_id(0)

    @pl.when(step == 0)
    def _():
        total[...] = jnp.zeros_like(total)

    row_at = lax.broadcasted_iota(jnp.int32, (128, 24), 0)
    lane_at = lax.broadcasted_iota(jnp.int32, (24, 128), 1)

    def group(index, carry):
        first = index * UNROLL
        spread = []
        drives = []
        for k in range(UNROLL):
            at = first + k
            start = block_ref[step * E_STEP + at] * 128
            hits = (dofs_ref[at] == row_at + start).astype(F32).astype(BF)
            table = table_ref[at]
            spread.append(jnp.dot(hits, table, preferred_element_type=F32))
            here = lane_at == var_ref[step * E_STEP + at] % 128
            drive = 0.0
            for p in range(2):
                piece = table[:, 24 + p : 25 + p].astype(F32)
                piece = jnp.where(here, piece, 0.0).astype(BF)
                drive += jnp.dot(hits, piece, preferred_element_type=F32)
            drives.append(drive)
        for k in range(UNROLL):
            at = first + k
            start = pl.multiple_of(block_ref[step * E_STEP + at] * 128, 128)
            rows = pl.ds(start, 128)
            part = jnp.dot(spread[k][:, :24].astype(BF), sens_ref[at], preferred_element_type=F32)
            total[rows, :] += part
            var = var_ref[step * E_STEP + at]
            tile = pl.ds(pl.multiple_of((var // 128) * 128, 128), 128)
            total[rows, tile] += drives[k]
        return carry

    lax.fori_loop(0, E_STEP // UNROLL, group, 0)

    @pl.when(step == pl.num_programs(0) - 1)
    def _():
        def turn(block, carry):
            rows = pl.ds(pl.multiple_of(block * 128, 128), 128)
            for q in range(4):
                tile = total[rows, q * 128 : q * 128 + 128].astype(BF).T
                for k in range(4):
                    out_ref[k % 2, 2 * q + k // 2, :, rows] = tile[k * 32 : k * 32 + 32]
            return carry

        lax.fori_loop(0, LR // 128, turn, 0)


def form_loads(tables, derivs, disps, sens_block, variables, places):
    drive = jnp.sum(derivs.astype(F32) * disps.astype(F32)[None], axis=1)
    high = lax.reduce_precision(drive, 8, 7)
    extra = -jnp.stack([high, drive - high], 1).astype(BF)
    fill = jnp.zeros((24, 6, 128), BF)
    table = jnp.concatenate([-tables, extra, fill], 1).transpose(2, 0, 1)
    blocks = jnp.minimum(jnp.min(places, axis=0) // 128, LR // 128 - 1)
    dofs = places.T[:, None, :]
    smem = pl.BlockSpec(memory_space=pltpu.SMEM)
    return pl.pallas_call(
        loads_kernel,
        grid=(128 // E_STEP,),
        in_specs=[
            smem,
            smem,
            pl.BlockSpec((E_STEP, 1, 24), lambda i: (i, 0, 0)),
            pl.BlockSpec((E_STEP, 24, 32), lambda i: (i, 0, 0)),
            pl.BlockSpec((E_STEP, 24, NRHS), lambda i: (i, 0, 0)),
        ],
        out_specs=pl.BlockSpec((2, 8, 32, LR), lambda i: (0, 0, 0, 0)),
        out_shape=jax.ShapeDtypeStruct((2, 8, 32, LR), BF),
        scratch_shapes=[pltpu.VMEM((LR, NRHS), F32)],
        cost_estimate=pl.CostEstimate(flops=800_000_000, bytes_accessed=8_000_000, transcendentals=0),
        name="loads",
    )(blocks, variables, dofs, table, sens_block)


def body(
    elem_mat,
    elem_deriv,
    elem_disp,
    elem_sens,
    design_var,
    dof_rows,
    inverse_factor,
    coupling,
    front_sizes,
):
    z = lax.axis_index(Z)
    c = lax.axis_index(C)
    h = lax.axis_index(H)
    l = lax.axis_index(L)
    x = lax.axis_index(X)
    core_swap = [(0, 1), (1, 0)]

    w_own, g_own = inverse_factor, coupling
    w_other = lax.ppermute(w_own, C, core_swap)
    g_other = lax.ppermute(g_own, C, core_swap)

    def turned(value):
        return jnp.where(c == 0, value, jnp.concatenate([value[:, 512:], value[:, :512]], 1))

    count = lax.iota(jnp.int32, 1024)
    block_rows = z * 1024 + jnp.where(c == 0, count, count ^ 512)

    def mask_of(front, rows):
        size = lax.dynamic_index_in_dim(front_sizes, front, 0, keepdims=False)
        return (rows < size).astype(F32)[None, :]

    place = l * 4 + x
    mask0 = mask_of(h * 2 + l, block_rows)
    mask0f = mask_of(h * 2 + l, x * 2048 + lax.iota(jnp.int32, 2048))
    mask1 = mask_of(4 + h, block_rows)
    mask1f = mask_of(4 + h, place * 1024 + count)
    mask2 = mask_of(6, block_rows)
    mask2f = mask_of(6, h * 4096 + place * 512 + lax.iota(jnp.int32, 512))

    def times_w(rhs, first, last):
        return dot_t(rhs[:, :512], w_own[first:last]) + dot_t(rhs[:, 512:], w_other[first:last])

    def times_wt(back, first, last):
        parts = [dot(back, w[first:last]).astype(BF) for w in (w_own, w_other)]
        return jnp.concatenate(parts, 1)

    def times_g(y, first, last):
        parts = [dot_t(y, g[:, first:last]).astype(BF) for g in (g_own, g_other)]
        return jnp.concatenate(parts, 1)

    def times_gt(parent, first, last):
        return dot(parent[:, :512], g_own[:, first:last]) + dot(parent[:, 512:], g_other[:, first:last])

    def by_front(value):
        return value.reshape(8, 2, 16, 1024).transpose(1, 0, 2, 3).reshape(16, 16, 1024)

    def from_front(value):
        return value.reshape(2, 8, 16, 1024).transpose(1, 0, 2, 3).reshape(256, 1024)

    halves = form_loads(elem_mat, elem_deriv, elem_disp, elem_sens, design_var, dof_rows)
    halves = exchange(halves, C).astype(F32)
    half = (halves[0] + halves[1]).astype(BF)
    top = exchange(half[:, :, :2048].reshape(4, 64, 2048), X)

    def halved(value, bit):
        pairs = value.reshape(-1, 2, 32, 1536)
        is_low = ((z >> bit) & 1) == 0
        kept = jnp.where(is_low, pairs[:, 0], pairs[:, 1])
        sent = jnp.where(is_low, pairs[:, 1], pairs[:, 0]).astype(BF)
        perm = [(at, at ^ (1 << bit)) for at in range(8)]
        return kept.astype(F32) + lax.ppermute(sent, Z, perm).astype(F32)

    rest = halved(half[:, :, 2048:], 0)
    top, rest = lax.optimization_barrier((top, rest))
    top = top.reshape(4, 64, 2, 1024).transpose(0, 2, 1, 3).reshape(8, 64, 1024)
    load0 = turned(reduce_chunks(top, Z))
    rhs0 = gather_chunks((mask0 * load0).astype(BF), X, 4).reshape(256, 1024)
    rest = halved(halved(rest, 1), 2)[0]
    rhs0, rest = lax.optimization_barrier((rhs0, rest))
    turn = [(zz * 8 + ss, ss * 8 + zz) for zz in range(8) for ss in range(8)]
    load1 = turned(lax.ppermute(rest[:, :1024], (Z, L, X), turn))
    rest2 = rest[:, 1024:].reshape(2, 16, 512)
    is_even = (x & 1) == 0
    got = []
    for k in range(2):
        sent = jnp.where(is_even, rest2[k], rest2[1 - k])
        perm = [
            (zz * 16 + ff, (ff >> 1) * 16 + ((ff & 1) ^ k) * 8 + zz)
            for zz in range(8)
            for ff in range(16)
        ]
        got.append(lax.ppermute(sent, (Z, H, L, X), perm))
    load2 = pair_up((h ^ c) == 0, got[0], got[1], 1)

    y0 = mask0f * reduce_chunks(times_w(rhs0, 0, 2048).reshape(8, 32, 2048), Z)
    y0, load1, load2 = lax.optimization_barrier((y0, load1, load2))
    y0_all = gather_chunks(y0.astype(BF), Z, 8).reshape(256, 2048)
    acc0 = reduce_chunks(times_g(y0_all, 0, 2048).reshape(8, 32, 1024), PAIR)

    rhs1 = gather_chunks((mask1 * (load1 - acc0)).astype(BF), PAIR, 8).reshape(256, 1024)
    y1 = mask1f * reduce_chunks(times_w(rhs1, 2048, 3072).reshape(8, 32, 1024), Z)
    y1_all = gather_chunks(y1.astype(BF), Z, 8).reshape(256, 1024)
    acc1 = reduce_chunks(by_front(times_g(y1_all, 2048, 3072)), FRONT)

    rhs2 = from_front(gather_chunks((mask2 * (load2 - acc1)).astype(BF), FRONT, 16))
    y2 = mask2f * reduce_chunks(times_w(rhs2, 3072, 3584).reshape(8, 32, 512), Z)
    back2 = gather_chunks(y2.astype(BF), Z, 8).reshape(256, 512)
    x2 = mask2 * reduce_chunks(by_front(times_wt(back2, 3072, 3584)), FRONT)
    got = []
    for k in range(2):
        sent = jnp.where((h ^ k ^ c) == 0, x2[:, :512], x2[:, 512:])
        perm = [
            (zz * 16 + ff, (ff & 7) * 16 + 2 * zz + ((ff >> 3) ^ k))
            for zz in range(8)
            for ff in range(16)
        ]
        got.append(lax.ppermute(sent, (Z, H, L, X), perm))
    out2 = pair_up(is_even, got[0], got[1], 0)
    x2_all = from_front(gather_chunks(x2.astype(BF), FRONT, 16))

    z1 = y1 - reduce_chunks(times_gt(x2_all, 2048, 3072).reshape(8, 32, 1024), Z)
    back1 = gather_chunks((mask1f * z1).astype(BF), Z, 8).reshape(256, 1024)
    x1 = mask1 * reduce_chunks(times_wt(back1, 2048, 3072).reshape(8, 32, 1024), PAIR)
    out1 = lax.ppermute(turned(x1), (Z, L, X), turn)
    x1_all = gather_chunks(x1.astype(BF), PAIR, 8).reshape(256, 1024)

    z0 = y0 - reduce_chunks(times_gt(x1_all, 0, 2048).reshape(8, 32, 2048), Z)
    back0 = gather_chunks((mask0f * z0).astype(BF), Z, 8).reshape(256, 2048)
    x0 = mask0 * reduce_chunks(times_wt(back0, 0, 2048).reshape(4, 64, 1024), X)
    x0 = turned(x0).reshape(2, 32, 1024)
    got = []
    for k in range(2):
        sent = jnp.where(((z & 1) ^ k) == 0, x0[0], x0[1])
        perm = [
            (zz * 4 + xx, (2 * xx + ((zz & 1) ^ k)) * 4 + (zz >> 1))
            for zz in range(8)
            for xx in range(4)
        ]
        got.append(lax.ppermute(sent, (Z, X), perm))
    out0 = pair_up((z & 1) == 0, got[0], got[1], 1)
    return jnp.concatenate([out0, out1, out2], 1).T


def solution(mesh):
    fine = Mesh(mesh.devices.reshape(8, 2, 2, 2, 4), (Z, C, H, L, X))
    elem, front = (Z, C), (H, L, X)
    both = elem + front
    return jax.shard_map(
        body,
        mesh=fine,
        in_specs=(
            P(None, None, both),
            P(None, None, both),
            P(None, both),
            P(both, None, None),
            P(both),
            P(None, both),
            P(front, elem),
            P(elem, front),
            P(),
        ),
        out_specs=P(front, elem),
        check_vma=False,
    )
```

```python
import jax
import jax.numpy as jnp
from jax import lax
from jax.experimental import pallas as pl
from jax.experimental.pallas import tpu as pltpu
from jax.sharding import Mesh
from jax.sharding import PartitionSpec as P

LR = 3584
NRHS = 512
BF = jnp.bfloat16
F32 = jnp.float32
E_STEP = 16
UNROLL = 8

Z, C, H, L, X = "z", "c", "h", "l", "x"
FRONT = (H, L, X)
PAIR = (L, X)


def dot_t(a, b):
    return lax.dot_general(a, b, (((1,), (1,)), ((), ())), preferred_element_type=F32)


def dot(a, b):
    return lax.dot_general(a, b, (((1,), (0,)), ((), ())), preferred_element_type=F32)


def exchange(chunks, axes):
    return lax.all_to_all(chunks, axes, split_axis=0, concat_axis=0, tiled=True)


def reduce_chunks(chunks, axes):
    return jnp.sum(exchange(chunks.astype(BF), axes).astype(F32), axis=0)


def gather_chunks(chunk, axes, count):
    return exchange(jnp.broadcast_to(chunk[None], (count,) + chunk.shape), axes)


def pair_up(is_first, own, other, axis):
    first = jnp.where(is_first, own, other)
    second = jnp.where(is_first, other, own)
    return jnp.concatenate([first, second], axis)


def loads_kernel(block_ref, var_ref, dofs_ref, table_ref, sens_ref, out_ref, total):
    step = pl.program_id(0)

    @pl.when(step == 0)
    def _():
        total[...] = jnp.zeros_like(total)

    row_at = lax.broadcasted_iota(jnp.int32, (128, 24), 0)
    lane_at = lax.broadcasted_iota(jnp.int32, (24, 128), 1)

    def group(index, carry):
        first = index * UNROLL
        spread = []
        drives = []
        for k in range(UNROLL):
            at = first + k
            start = block_ref[step * E_STEP + at] * 128
            hits = (dofs_ref[at] == row_at + start).astype(F32).astype(BF)
            table = table_ref[at]
            spread.append(jnp.dot(hits, table, preferred_element_type=F32))
            here = lane_at == var_ref[step * E_STEP + at] % 128
            drive = 0.0
            for p in range(2):
                piece = table[:, 24 + p : 25 + p].astype(F32)
                piece = jnp.where(here, piece, 0.0).astype(BF)
                drive += jnp.dot(hits, piece, preferred_element_type=F32)
            drives.append(drive)
        for k in range(UNROLL):
            at = first + k
            start = pl.multiple_of(block_ref[step * E_STEP + at] * 128, 128)
            rows = pl.ds(start, 128)
            part = jnp.dot(spread[k][:, :24].astype(BF), sens_ref[at], preferred_element_type=F32)
            total[rows, :] += part
            var = var_ref[step * E_STEP + at]
            tile = pl.ds(pl.multiple_of((var // 128) * 128, 128), 128)
            total[rows, tile] += drives[k]
        return carry

    lax.fori_loop(0, E_STEP // UNROLL, group, 0)

    @pl.when(step == pl.num_programs(0) - 1)
    def _():
        def turn(block, carry):
            rows = pl.ds(pl.multiple_of(block * 128, 128), 128)
            for q in range(4):
                tile = total[rows, q * 128 : q * 128 + 128].astype(BF).T
                for k in range(4):
                    out_ref[k % 2, 2 * q + k // 2, :, rows] = tile[k * 32 : k * 32 + 32]
            return carry

        lax.fori_loop(0, LR // 128, turn, 0)


def form_loads(tables, derivs, disps, sens_block, variables, places):
    drive = jnp.sum(derivs.astype(F32) * disps.astype(F32)[None], axis=1)
    high = lax.reduce_precision(drive, 8, 7)
    extra = -jnp.stack([high, drive - high], 1).astype(BF)
    fill = jnp.zeros((24, 6, 128), BF)
    table = jnp.concatenate([-tables, extra, fill], 1).transpose(2, 0, 1)
    blocks = jnp.minimum(jnp.min(places, axis=0) // 128, LR // 128 - 1)
    dofs = places.T[:, None, :]
    smem = pl.BlockSpec(memory_space=pltpu.SMEM)
    return pl.pallas_call(
        loads_kernel,
        grid=(128 // E_STEP,),
        in_specs=[
            smem,
            smem,
            pl.BlockSpec((E_STEP, 1, 24), lambda i: (i, 0, 0)),
            pl.BlockSpec((E_STEP, 24, 32), lambda i: (i, 0, 0)),
            pl.BlockSpec((E_STEP, 24, NRHS), lambda i: (i, 0, 0)),
        ],
        out_specs=pl.BlockSpec((2, 8, 32, LR), lambda i: (0, 0, 0, 0)),
        out_shape=jax.ShapeDtypeStruct((2, 8, 32, LR), BF),
        scratch_shapes=[pltpu.VMEM((LR, NRHS), F32)],
        cost_estimate=pl.CostEstimate(flops=800_000_000, bytes_accessed=8_000_000, transcendentals=0),
        name="loads",
    )(blocks, variables, dofs, table, sens_block)


def body(
    elem_mat,
    elem_deriv,
    elem_disp,
    elem_sens,
    design_var,
    dof_rows,
    inverse_factor,
    coupling,
    front_sizes,
):
    z = lax.axis_index(Z)
    c = lax.axis_index(C)
    h = lax.axis_index(H)
    l = lax.axis_index(L)
    x = lax.axis_index(X)
    core_swap = [(0, 1), (1, 0)]

    w_own, g_own = inverse_factor, coupling
    w_other = lax.ppermute(w_own, C, core_swap)
    g_other = lax.ppermute(g_own, C, core_swap)

    def turned(value):
        return jnp.where(c == 0, value, jnp.concatenate([value[:, 512:], value[:, :512]], 1))

    count = lax.iota(jnp.int32, 1024)
    block_rows = z * 1024 + jnp.where(c == 0, count, count ^ 512)

    def mask_of(front, rows):
        size = lax.dynamic_index_in_dim(front_sizes, front, 0, keepdims=False)
        return (rows < size).astype(F32)[None, :]

    place = l * 4 + x
    mask0 = mask_of(h * 2 + l, block_rows)
    mask0f = mask_of(h * 2 + l, x * 2048 + lax.iota(jnp.int32, 2048))
    mask1 = mask_of(4 + h, block_rows)
    mask1f = mask_of(4 + h, place * 1024 + count)
    mask2 = mask_of(6, block_rows)
    mask2f = mask_of(6, h * 4096 + place * 512 + lax.iota(jnp.int32, 512))

    def times_w(rhs, first, last):
        return dot_t(rhs[:, :512], w_own[first:last]) + dot_t(rhs[:, 512:], w_other[first:last])

    def times_wt(back, first, last):
        parts = [dot(back, w[first:last]).astype(BF) for w in (w_own, w_other)]
        return jnp.concatenate(parts, 1)

    def times_g(y, first, last):
        parts = [dot_t(y, g[:, first:last]).astype(BF) for g in (g_own, g_other)]
        return jnp.concatenate(parts, 1)

    def times_gt(parent, first, last):
        return dot(parent[:, :512], g_own[:, first:last]) + dot(parent[:, 512:], g_other[:, first:last])

    def by_front(value):
        return value.reshape(8, 2, 16, 1024).transpose(1, 0, 2, 3).reshape(16, 16, 1024)

    def from_front(value):
        return value.reshape(2, 8, 16, 1024).transpose(1, 0, 2, 3).reshape(256, 1024)

    halves = form_loads(elem_mat, elem_deriv, elem_disp, elem_sens, design_var, dof_rows)
    halves = exchange(halves, C)
    half = halves[0] + halves[1]
    top = exchange(half[:, :, :2048].reshape(4, 64, 2048), X)

    def halved(value, bit):
        pairs = value.reshape(-1, 2, 32, 1536)
        is_low = ((z >> bit) & 1) == 0
        kept = jnp.where(is_low, pairs[:, 0], pairs[:, 1])
        sent = jnp.where(is_low, pairs[:, 1], pairs[:, 0]).astype(BF)
        perm = [(at, at ^ (1 << bit)) for at in range(8)]
        return kept.astype(F32) + lax.ppermute(sent, Z, perm).astype(F32)

    rest = halved(half[:, :, 2048:], 0)
    top, rest = lax.optimization_barrier((top, rest))
    top = top.reshape(4, 64, 2, 1024).transpose(0, 2, 1, 3).reshape(8, 64, 1024)
    load0 = turned(reduce_chunks(top, Z))
    rhs0 = gather_chunks((mask0 * load0).astype(BF), X, 4).reshape(256, 1024)
    rest = halved(halved(rest, 1), 2)[0]
    rhs0, rest = lax.optimization_barrier((rhs0, rest))
    turn = [(zz * 8 + ss, ss * 8 + zz) for zz in range(8) for ss in range(8)]
    load1 = turned(lax.ppermute(rest[:, :1024], (Z, L, X), turn))
    rest2 = rest[:, 1024:].reshape(2, 16, 512)
    is_even = (x & 1) == 0
    got = []
    for k in range(2):
        sent = jnp.where(is_even, rest2[k], rest2[1 - k])
        perm = [
            (zz * 16 + ff, (ff >> 1) * 16 + ((ff & 1) ^ k) * 8 + zz)
            for zz in range(8)
            for ff in range(16)
        ]
        got.append(lax.ppermute(sent, (Z, H, L, X), perm))
    load2 = pair_up((h ^ c) == 0, got[0], got[1], 1)

    y0 = mask0f * reduce_chunks(times_w(rhs0, 0, 2048).reshape(8, 32, 2048), Z)
    y0, load1, load2 = lax.optimization_barrier((y0, load1, load2))
    y0_all = gather_chunks(y0.astype(BF), Z, 8).reshape(256, 2048)
    acc0 = reduce_chunks(times_g(y0_all, 0, 2048).reshape(8, 32, 1024), PAIR)

    rhs1 = gather_chunks((mask1 * (load1 - acc0)).astype(BF), PAIR, 8).reshape(256, 1024)
    y1 = mask1f * reduce_chunks(times_w(rhs1, 2048, 3072).reshape(8, 32, 1024), Z)
    y1_all = gather_chunks(y1.astype(BF), Z, 8).reshape(256, 1024)
    acc1 = reduce_chunks(by_front(times_g(y1_all, 2048, 3072)), FRONT)

    rhs2 = from_front(gather_chunks((mask2 * (load2 - acc1)).astype(BF), FRONT, 16))
    y2 = mask2f * reduce_chunks(times_w(rhs2, 3072, 3584).reshape(8, 32, 512), Z)
    back2 = gather_chunks(y2.astype(BF), Z, 8).reshape(256, 512)
    x2 = mask2 * reduce_chunks(by_front(times_wt(back2, 3072, 3584)), FRONT)
    got = []
    for k in range(2):
        sent = jnp.where((h ^ k ^ c) == 0, x2[:, :512], x2[:, 512:])
        perm = [
            (zz * 16 + ff, (ff & 7) * 16 + 2 * zz + ((ff >> 3) ^ k))
            for zz in range(8)
            for ff in range(16)
        ]
        got.append(lax.ppermute(sent, (Z, H, L, X), perm))
    out2 = pair_up(is_even, got[0], got[1], 0)
    x2_all = from_front(gather_chunks(x2.astype(BF), FRONT, 16))

    z1 = y1 - reduce_chunks(times_gt(x2_all, 2048, 3072).reshape(8, 32, 1024), Z)
    back1 = gather_chunks((mask1f * z1).astype(BF), Z, 8).reshape(256, 1024)
    x1 = mask1 * reduce_chunks(times_wt(back1, 2048, 3072).reshape(8, 32, 1024), PAIR)
    out1 = lax.ppermute(turned(x1), (Z, L, X), turn)
    x1_all = gather_chunks(x1.astype(BF), PAIR, 8).reshape(256, 1024)

    z0 = y0 - reduce_chunks(times_gt(x1_all, 0, 2048).reshape(8, 32, 2048), Z)
    back0 = gather_chunks((mask0f * z0).astype(BF), Z, 8).reshape(256, 2048)
    x0 = mask0 * reduce_chunks(times_wt(back0, 0, 2048).reshape(4, 64, 1024), X)
    x0 = turned(x0).reshape(2, 32, 1024)
    got = []
    for k in range(2):
        sent = jnp.where(((z & 1) ^ k) == 0, x0[0], x0[1])
        perm = [
            (zz * 4 + xx, (2 * xx + ((zz & 1) ^ k)) * 4 + (zz >> 1))
            for zz in range(8)
            for xx in range(4)
        ]
        got.append(lax.ppermute(sent, (Z, X), perm))
    out0 = pair_up((z & 1) == 0, got[0], got[1], 1)
    return jnp.concatenate([out0, out1, out2], 1).T


def solution(mesh):
    fine = Mesh(mesh.devices.reshape(8, 2, 2, 2, 4), (Z, C, H, L, X))
    elem, front = (Z, C), (H, L, X)
    both = elem + front
    return jax.shard_map(
        body,
        mesh=fine,
        in_specs=(
            P(None, None, both),
            P(None, None, both),
            P(None, both),
            P(both, None, None),
            P(both),
            P(None, both),
            P(front, elem),
            P(elem, front),
            P(),
        ),
        out_specs=P(front, elem),
        check_vma=False,
    )
```
